32 devices in a mesh: gx: 8 (over y, x, core), gy: 4 (over z).
Axes of the slice: x: 2, y: 2, z: 4, core: 2. Of those that a mesh axis runs over, the one named last changes fastest.
Arguments:
- layer_early: bfloat16 [1024, 8192], P(None, ('gx', 'gy')), may hold values from -48 to 48
- layer_late: bfloat16 [1024, 8192], P(('gx', 'gy')), may hold values from -48 to 48
Outputs:
- similarity: float32 [], replicated
- token_share: float32 [1024], P(('gx', 'gy'))
- early_rows: bfloat16 [1024, 8192], P(('gx', 'gy'))
- late_rows: bfloat16 [1024, 8192], P(('gx', 'gy'))
The draws below stay inside these ranges and needn't reach their ends.
All inputs are finite; a program needn't handle non-finite values.
Results may differ from the reference program's by a relative error of at most 0.0015.
Values may be sent and summed in bfloat16 or wider, within the bound.
A program may use at most 128 MiB of HBM per device.

```python
import math
import jax
import jax.numpy as jnp
from jax import lax

D = 8192
TOKENS = 1024


def draw_layer(key, salt):
    order = jax.random.permutation(jax.random.fold_in(key, 5), D)
    spectrum = 6.0 * jnp.power(order.astype(jnp.float32) + 1.0, -0.5)
    jitter = jnp.exp(jax.random.uniform(jax.random.fold_in(key, salt + 3), (D,), jnp.float32, minval=math.log(0.5), maxval=math.log(2.0)))
    column_scale = jnp.sqrt(spectrum * jitter)
    shared = jax.random.normal(jax.random.fold_in(key, 7), (TOKENS, D), jnp.float32)
    own_part = jax.random.normal(jax.random.fold_in(key, salt + 1), (TOKENS, D), jnp.float32)
    offsets = jax.random.uniform(jax.random.fold_in(key, salt + 2), (D,), jnp.float32, minval=-8.0, maxval=8.0)
    signal = (0.9 * shared + 0.436 * own_part) * column_scale
    return jnp.clip(signal + offsets, -48.0, 48.0)


def draw_layer_early(key, part):
    return draw_layer(key, 11).astype(jnp.bfloat16)


def draw_layer_late(key, part):
    return draw_layer(key, 23).astype(jnp.bfloat16)


def setup_inputs(seed: int = 0) -> dict:
    splits = jax.random.split(jax.random.key(seed), 3)
    layer_early = draw_layer_early(jax.random.fold_in(splits[2], 71), 0)
    layer_late = draw_layer_late(jax.random.fold_in(splits[2], 71), 0)
    return {"layer_early": layer_early, "layer_late": layer_late}


def reference(layer_early, layer_late):
    early_values = layer_early.astype(jnp.float32)
    late_values = layer_late.astype(jnp.float32)
    early_rows = (early_values - lax.optimization_barrier(jnp.mean(early_values, axis=0))).astype(jnp.bfloat16)
    late_rows = (late_values - lax.optimization_barrier(jnp.mean(late_values, axis=0))).astype(jnp.bfloat16)
    gram_early = jnp.dot(early_rows, early_rows.T, preferred_element_type=jnp.float32)
    gram_late = jnp.dot(late_rows, late_rows.T, preferred_element_type=jnp.float32)
    row_align = lax.optimization_barrier(jnp.sum(gram_early * gram_late, axis=1))
    hsic_kl = jnp.sum(row_align)
    hsic_kk = jnp.sum(gram_early * gram_early)
    hsic_ll = jnp.sum(gram_late * gram_late)
    scale_norm = jnp.sqrt(hsic_kk * hsic_ll)
    similarity = hsic_kl / scale_norm
    token_share = TOKENS * row_align / scale_norm
    return (similarity, token_share, early_rows, late_rows)
```

```python
import functools

import jax
import jax.numpy as jnp
from jax import lax
from jax.experimental import pallas as pl
from jax.experimental.pallas import tpu as pltpu
from jax.sharding import PartitionSpec as P

MESH = pl.DeviceIdType.MESH
NT = (((1,), (1,)), ((), ()))
VMEM_BUDGET = 48 * 2**20


def pair_terms(left_early, left_late, right_early, right_late):
    block_early = lax.dot_general(left_early, right_early, NT, preferred_element_type=jnp.float32)
    block_late = lax.dot_general(left_late, right_late, NT, preferred_element_type=jnp.float32)
    return (
        jnp.sum(block_early * block_late, axis=1),
        jnp.sum(block_early * block_early),
        jnp.sum(block_late * block_late),
    )


def gather_body(layer_early, layer_late):
    total_rows = layer_early.shape[0]
    early_values = layer_early.astype(jnp.float32)
    early_cols = (early_values - jnp.mean(early_values, axis=0)).astype(jnp.bfloat16)
    late_values = layer_late.astype(jnp.float32)
    column_sums = lax.psum(jnp.sum(late_values, axis=0), ("gx", "gy"))
    late_rows = (late_values - column_sums / total_rows).astype(jnp.bfloat16)
    early_rows = lax.all_to_all(early_cols, ("gx", "gy"), split_axis=0, concat_axis=1, tiled=True)
    block_early, block_late = (
        lax.all_gather(early_rows, "gy", axis=0, tiled=True),
        lax.all_gather(late_rows, "gy", axis=0, tiled=True),
    )
    row_part, early_part, late_part = pair_terms(
        block_early,
        block_late,
        lax.all_gather(early_rows, "gx", axis=0, tiled=True),
        lax.all_gather(late_rows, "gx", axis=0, tiled=True),
    )
    own_align = lax.psum_scatter(row_part, "gy", scatter_dimension=0, tiled=True)
    total_kl, total_kk, total_ll = lax.psum(
        (jnp.sum(row_part), early_part, late_part), ("gx", "gy")
    )
    scale_norm = jnp.sqrt(total_kk * total_ll)
    similarity = total_kl / scale_norm
    token_share = total_rows * own_align / scale_norm
    return (similarity, token_share, early_rows, late_rows)


def kernel(gx, gy, early_ref, late_ref, early_out, late_out, small_out,
           early_pair, late_pair, means,
           early_send, early_recv, early_own, late_send, late_recv, late_own,
           early_zsend, early_zrecv, late_zsend, late_zrecv,
           msg, msg_recv,
           a2a_send, a2a_recv, own_sem, pair_send, pair_recv, mean_send, mean_recv,
           plane_send, plane_recv, z_send, z_recv, msg_send, msg_recv_sem):
    n = gx * gy
    tokens, cols = early_ref.shape
    rows = late_ref.shape[0]
    block = tokens // gx
    half = gx // 2
    x, y = lax.axis_index("gx"), lax.axis_index("gy")
    me = x * gy + y
    core = lax.rem(x, 2)
    chip = x // 2
    partner = x + 1 - 2 * core

    def device(t):
        return (t // gy, lax.rem(t, gy))

    def lanes(i):
        return pl.ds(pl.multiple_of(i * cols, cols), cols)

    def tile_rows(i, size):
        return pl.ds(pl.multiple_of(i * size, size), size)

    def others(f):
        def step(o, carry):
            f(lax.rem(me + o, n))
            return carry
        lax.fori_loop(1, n, step, 0)

    def wait_bytes(ref, sem):
        pltpu.make_async_copy(ref, ref, sem).wait()

    barrier = pltpu.get_barrier_semaphore()
    others(lambda t: pl.semaphore_signal(barrier, inc=1, device_id=device(t), device_id_type=MESH))
    pl.semaphore_wait(barrier, n - 1)

    own_rows = tile_rows(me, rows)

    others(lambda t: pltpu.make_async_remote_copy(
        src_ref=late_ref.at[:, lanes(t)], dst_ref=late_pair.at[own_rows, pl.ds(0, cols)],
        send_sem=a2a_send.at[0], recv_sem=a2a_recv.at[0],
        device_id=device(t), device_id_type=MESH).start())
    late_pair[own_rows, pl.ds(0, cols)] = late_ref[:, lanes(me)]

    values = early_ref[...].astype(jnp.float32)
    mean = jnp.sum(values, axis=0, keepdims=True) / tokens
    early_pair[:, pl.ds(0, cols)] = (values - mean).astype(jnp.bfloat16)

    def swap(pair, i):
        return pltpu.make_async_remote_copy(
            src_ref=pair.at[:, pl.ds(0, cols)], dst_ref=pair.at[:, pl.ds(cols, cols)],
            send_sem=pair_send.at[i], recv_sem=pair_recv.at[i],
            device_id=(partner, y), device_id_type=MESH)

    early_swap = swap(early_pair, 0)
    early_swap.start()

    def gram_pieces(pair, own, send, recv, i):
        copies = []
        for o in list(range(1, half)) + [0]:
            q = 2 * lax.rem(chip + o, half) + core
            left = pair[tile_rows(q, block), :]
            right = jnp.concatenate(
                [pair[tile_rows(lax.rem(q + d, gx), block), :] for d in range(half + 1)], axis=0)
            piece = lax.dot_general(left, right, NT, preferred_element_type=jnp.float32)
            if o == 0:
                own[...] = piece
            else:
                send[o - 1] = piece.astype(jnp.bfloat16)
                copy = pltpu.make_async_remote_copy(
                    src_ref=send.at[o - 1], dst_ref=recv.at[o - 1],
                    send_sem=plane_send.at[i, o - 1], recv_sem=plane_recv.at[i, o - 1],
                    device_id=(q, y), device_id_type=MESH)
                copy.start()
                copies.append(copy)
        return copies

    def along_z(copies, own, recv, zsend, zrecv, i):
        total = own[...]
        for o, copy in enumerate(copies):
            copy.wait_recv()
            total = total + recv[o].astype(jnp.float32)
        own[...] = total
        zsend[...] = total.astype(jnp.bfloat16)
        out = []
        for o in range(1, gy):
            z = lax.rem(y + o, gy)
            copy = pltpu.make_async_remote_copy(
                src_ref=zsend.at[tile_rows(z, rows), :], dst_ref=zrecv.at[o - 1],
                send_sem=z_send.at[i, o - 1], recv_sem=z_recv.at[i, o - 1],
                device_id=(x, z), device_id_type=MESH)
            copy.start()
            out.append(copy)
        return out

    early_swap.wait_recv()
    early_copies = gram_pieces(early_pair, early_own, early_send, early_recv, 0)

    others(lambda t: pltpu.make_async_remote_copy(
        src_ref=early_pair.at[tile_rows(t, rows), pl.ds(0, cols)], dst_ref=early_out.at[:, lanes(me)],
        send_sem=a2a_send.at[1], recv_sem=a2a_recv.at[1],
        device_id=device(t), device_id_type=MESH).start())
    own_copy = pltpu.make_async_copy(
        early_pair.at[own_rows, pl.ds(0, cols)], early_out.at[:, lanes(me)], own_sem)
    own_copy.start()

    wait_bytes(late_pair.at[pl.ds(0, tokens - rows), pl.ds(0, cols)], a2a_recv.at[0])
    values = late_pair[:, pl.ds(0, cols)].astype(jnp.float32)
    mean = jnp.sum(values, axis=0, keepdims=True) / tokens
    late_pair[:, pl.ds(0, cols)] = (values - mean).astype(jnp.bfloat16)
    late_swap = swap(late_pair, 1)
    late_swap.start()
    means[:, lanes(me)] = mean
    others(lambda t: pltpu.make_async_remote_copy(
        src_ref=means.at[:, lanes(me)], dst_ref=means.at[:, lanes(me)],
        send_sem=mean_send, recv_sem=mean_recv,
        device_id=device(t), device_id_type=MESH).start())

    late_swap.wait_recv()
    late_copies = gram_pieces(late_pair, late_own, late_send, late_recv, 1)
    early_z = along_z(early_copies, early_own, early_recv, early_zsend, early_zrecv, 0)
    wait_bytes(means.at[:, pl.ds(0, (n - 1) * cols)], mean_recv)
    late_out[...] = (late_ref[...].astype(jnp.float32) - means[...]).astype(jnp.bfloat16)
    late_z = along_z(late_copies, late_own, late_recv, late_zsend, late_zrecv, 1)

    def final(copies, own, zrecv):
        total = own[tile_rows(y, rows), :]
        for o, copy in enumerate(copies):
            copy.wait_recv()
            total = total + zrecv[o].astype(jnp.float32)
        return total

    k = final(early_z, early_own, early_zrecv)
    l = final(late_z, late_own, late_zrecv)
    kl = k * l
    sub = lax.broadcasted_iota(jnp.int32, (rows, block), 0)
    lane = lax.broadcasted_iota(jnp.int32, (rows, block), 1)

    def weighted(v):
        doubled = jnp.sum(v[:, block:half * block])
        return jnp.sum(v[:, :block]) + jnp.sum(v[:, half * block:]) + 2.0 * doubled

    head = lax.broadcasted_iota(jnp.int32, (1, block), 1)
    scalars = jnp.where(head == 0, weighted(kl), jnp.where(
        head == 1, weighted(k * k), jnp.where(head == 2, weighted(l * l), 0.0)))
    for d in range(gx):
        if 0 < d < half:
            top = jnp.sum(kl[:, d * block:(d + 1) * block], axis=0, keepdims=True)
        else:
            top = jnp.zeros((1, block), jnp.float32)
        msg[d] = jnp.concatenate([top, scalars], axis=0)
    msg_recv[me] = msg[0]
    others(lambda t: pltpu.make_async_remote_copy(
        src_ref=msg.at[lax.rem(t // gy - x + gx, gx)], dst_ref=msg_recv.at[me],
        send_sem=msg_send, recv_sem=msg_recv_sem,
        device_id=device(t), device_id_type=MESH).start())
    own_align = jnp.sum(kl, axis=1, keepdims=True)
    wait_bytes(msg_recv.at[pl.ds(0, n - 1)], msg_recv_sem)
    got = jnp.sum(msg_recv[...], axis=0)
    below = jnp.sum(jnp.where(lane == y * rows + sub, got[0:1, :], 0.0), axis=1, keepdims=True)
    align = jnp.sum(jnp.where(lane == sub, own_align + below, 0.0), axis=0, keepdims=True)
    sums = got[1:2, :]
    total_kl = jnp.sum(jnp.where(head == 0, sums, 0.0), axis=1, keepdims=True)
    total_kk = jnp.sum(jnp.where(head == 1, sums, 0.0), axis=1, keepdims=True)
    total_ll = jnp.sum(jnp.where(head == 2, sums, 0.0), axis=1, keepdims=True)
    scale_norm = jnp.sqrt(total_kk * total_ll)
    small_out[0:1, :] = tokens * align / scale_norm
    small_out[1:2, :] = jnp.broadcast_to(total_kl / scale_norm, (1, block))

    part = late_pair.at[pl.ds(0, tokens - rows), pl.ds(0, cols)]
    wait_bytes(part, a2a_send.at[0])
    wait_bytes(part, a2a_send.at[1])
    wait_bytes(early_out.at[:, pl.ds(0, (n - 1) * cols)], a2a_recv.at[1])
    own_copy.wait()
    early_swap.wait_send()
    late_swap.wait_send()
    wait_bytes(means.at[:, pl.ds(0, (n - 1) * cols)], mean_send)
    wait_bytes(msg_recv.at[pl.ds(0, n - 1)], msg_send)
    for copy in early_copies + late_copies + early_z + late_z:
        copy.wait_send()


def exchange_body(gx, gy, layer_early, layer_late):
    tokens, cols = layer_early.shape
    rows, width = layer_late.shape
    n = gx * gy
    block = tokens // gx
    half = gx // 2
    span = (half + 1) * block
    bf16, f32 = jnp.bfloat16, jnp.float32
    dma = pltpu.SemaphoreType.DMA
    gram = [
        pltpu.VMEM((half - 1, block, span), bf16),
        pltpu.VMEM((half - 1, block, span), bf16),
        pltpu.VMEM((block, span), f32),
    ]
    z_part = [pltpu.VMEM((block, span), bf16), pltpu.VMEM((gy - 1, rows, span), bf16)]
    vmem = pl.BlockSpec(memory_space=pltpu.VMEM)
    early_rows, late_rows, small = pl.pallas_call(
        functools.partial(kernel, gx, gy),
        out_shape=(
            jax.ShapeDtypeStruct((rows, width), bf16),
            jax.ShapeDtypeStruct((rows, width), bf16),
            jax.ShapeDtypeStruct((2, block), f32),
        ),
        in_specs=[vmem, vmem],
        out_specs=(pl.BlockSpec(memory_space=pl.ANY), vmem, vmem),
        scratch_shapes=[
            pltpu.VMEM((tokens, 2 * cols), bf16),
            pltpu.VMEM((tokens, 2 * cols), bf16),
            pltpu.VMEM((1, width), f32),
            *gram, *gram, *z_part, *z_part,
            pltpu.VMEM((gx, 2, block), f32),
            pltpu.VMEM((n, 2, block), f32),
            dma((2,)), dma((2,)), dma, dma((2,)), dma((2,)), dma, dma,
            dma((2, half - 1)), dma((2, half - 1)), dma((2, gy - 1)), dma((2, gy - 1)), dma, dma,
        ],
        compiler_params=pltpu.CompilerParams(collective_id=0, has_side_effects=True),
    )(layer_early, layer_late)
    return small[1, 0], small[0, :rows], early_rows, late_rows


def fits(gx, gy, tokens, width):
    n = gx * gy
    cols, rows, block = width // n, tokens // n, tokens // gx
    aligned = cols % 128 == 0 and rows % 16 == 0 and block % 128 == 0
    span = (gx // 2 + 1) * block
    held = 12 * tokens * cols + 4 * gx * block * span + 24 * block * span
    return gx % 2 == 0 and gx >= 4 and gy >= 2 and aligned and rows <= block and held <= VMEM_BUDGET


def solution(mesh):
    gx, gy = mesh.shape["gx"], mesh.shape["gy"]

    def body(layer_early, layer_late):
        if fits(gx, gy, layer_early.shape[0], layer_late.shape[1]):
            return exchange_body(gx, gy, layer_early, layer_late)
        return gather_body(layer_early, layer_late)

    in_specs = (P(None, ("gx", "gy")), P(("gx", "gy"), None))
    out_specs = (P(), P(("gx", "gy")), P(("gx", "gy"), None), P(("gx", "gy"), None))
    return jax.shard_map(body, mesh=mesh, in_specs=in_specs, out_specs=out_specs, check_vma=False)
```

```python
import functools

import jax
import jax.numpy as jnp
from jax import lax
from jax.experimental import pallas as pl
from jax.experimental.pallas import tpu as pltpu
from jax.sharding import PartitionSpec as P

MESH = pl.DeviceIdType.MESH
NT = (((1,), (1,)), ((), ()))
VMEM_BUDGET = 48 * 2**20


def pair_terms(left_early, left_late, right_early, right_late):
    block_early = lax.dot_general(left_early, right_early, NT, preferred_element_type=jnp.float32)
    block_late = lax.dot_general(left_late, right_late, NT, preferred_element_type=jnp.float32)
    return (
        jnp.sum(block_early * block_late, axis=1),
        jnp.sum(block_early * block_early),
        jnp.sum(block_late * block_late),
    )


def gather_body(layer_early, layer_late):
    total_rows = layer_early.shape[0]
    early_values = layer_early.astype(jnp.float32)
    early_cols = (early_values - jnp.mean(early_values, axis=0)).astype(jnp.bfloat16)
    late_values = layer_late.astype(jnp.float32)
    column_sums = lax.psum(jnp.sum(late_values, axis=0), ("gx", "gy"))
    late_rows = (late_values - column_sums / total_rows).astype(jnp.bfloat16)
    early_rows = lax.all_to_all(early_cols, ("gx", "gy"), split_axis=0, concat_axis=1, tiled=True)
    block_early, block_late = (
        lax.all_gather(early_rows, "gy", axis=0, tiled=True),
        lax.all_gather(late_rows, "gy", axis=0, tiled=True),
    )
    row_part, early_part, late_part = pair_terms(
        block_early,
        block_late,
        lax.all_gather(early_rows, "gx", axis=0, tiled=True),
        lax.all_gather(late_rows, "gx", axis=0, tiled=True),
    )
    own_align = lax.psum_scatter(row_part, "gy", scatter_dimension=0, tiled=True)
    total_kl, total_kk, total_ll = lax.psum(
        (jnp.sum(row_part), early_part, late_part), ("gx", "gy")
    )
    scale_norm = jnp.sqrt(total_kk * total_ll)
    similarity = total_kl / scale_norm
    token_share = total_rows * own_align / scale_norm
    return (similarity, token_share, early_rows, late_rows)


def kernel(gx, gy, early_hbm, late_hbm, early_out, early_mean_out, late_mean_out, share_out, similarity_out,
           early_ref, late_ref, early_plane, early_pair, late_pair, means,
           early_send, early_recv, early_own, late_send, late_recv, late_own,
           early_zsend, early_zrecv, late_zsend, late_zrecv,
           diag_send, diag_recv, diag_zsend, diag_zrecv,
           msg, msg_recv,
           stage_sem, a2a_send, a2a_recv, own_sem, pair_send, pair_recv, mean_send, mean_recv,
           plane_send, plane_recv, z_send, z_recv, msg_send, msg_recv_sem,
           diag_plane_send, diag_plane_recv, diag_z_send, diag_z_recv, out_send, out_recv):
    n = gx * gy
    tokens, cols = early_ref.shape
    rows = late_ref.shape[0]
    block = tokens // gx
    half = gx // 2
    x, y = lax.axis_index("gx"), lax.axis_index("gy")
    me = x * gy + y
    core = lax.rem(x, 2)
    chip = x // 2
    partner = x + 1 - 2 * core

    def device(t):
        return (t // gy, lax.rem(t, gy))

    def lanes(i):
        return pl.ds(pl.multiple_of(i * cols, cols), cols)

    def tile_rows(i, size):
        return pl.ds(pl.multiple_of(i * size, size), size)

    def others(f):
        def step(o, carry):
            f(lax.rem(me + o, n))
            return carry
        lax.fori_loop(1, n, step, 0)

    def wait_bytes(ref, sem):
        pltpu.make_async_copy(ref, ref, sem).wait()

    barrier = pltpu.get_barrier_semaphore()
    others(lambda t: pl.semaphore_signal(barrier, inc=1, device_id=device(t), device_id_type=MESH))
    stage_late = pltpu.make_async_copy(late_hbm, late_ref, stage_sem.at[0])
    stage_late.start()
    stage_early = pltpu.make_async_copy(early_hbm, early_ref, stage_sem.at[1])
    stage_early.start()
    stage_late.wait()
    pl.semaphore_wait(barrier, n - 1)

    own_rows = tile_rows(me, rows)

    others(lambda t: pltpu.make_async_remote_copy(
        src_ref=late_ref.at[:, lanes(t)], dst_ref=late_pair.at[own_rows, pl.ds(0, cols)],
        send_sem=a2a_send.at[0], recv_sem=a2a_recv.at[0],
        device_id=device(t), device_id_type=MESH).start())
    late_pair[own_rows, pl.ds(0, cols)] = late_ref[:, lanes(me)]

    stage_early.wait()
    plane_copies = []
    for o in range(1, gx):
        p = lax.rem(x + o, gx)
        copy = pltpu.make_async_remote_copy(
            src_ref=early_ref.at[tile_rows(p, block), :], dst_ref=early_plane.at[:, lanes(x)],
            send_sem=out_send.at[o - 1], recv_sem=out_recv.at[o - 1],
            device_id=(p, y), device_id_type=MESH)
        copy.start()
        plane_copies.append(copy)
    early_plane[:, lanes(x)] = early_ref[tile_rows(x, block), :]

    values = early_ref[...].astype(jnp.float32)
    early_mean = jnp.sum(values, axis=0, keepdims=True) / tokens
    early_pair[:, pl.ds(0, cols)] = (values - early_mean).astype(jnp.bfloat16)

    def swap(pair, i):
        return pltpu.make_async_remote_copy(
            src_ref=pair.at[:, pl.ds(0, cols)], dst_ref=pair.at[:, pl.ds(cols, cols)],
            send_sem=pair_send.at[i], recv_sem=pair_recv.at[i],
            device_id=(partner, y), device_id_type=MESH)

    early_swap = swap(early_pair, 0)
    early_swap.start()

    def diagonal(v):
        on = (lax.broadcasted_iota(jnp.int32, (block, block), 0)
              == lax.broadcasted_iota(jnp.int32, (block, block), 1))
        return jnp.sum(jnp.where(on, v[:, :block], 0.0), axis=0, keepdims=True)

    def gram_pieces(pair, own, send, recv, i):
        copies, diag_copies = [], []
        for o in list(range(1, half)) + [0]:
            q = 2 * lax.rem(chip + o, half) + core
            left = pair[tile_rows(q, block), :]
            right = jnp.concatenate(
                [pair[tile_rows(lax.rem(q + d, gx), block), :] for d in range(half + 1)], axis=0)
            piece = lax.dot_general(left, right, NT, preferred_element_type=jnp.float32)
            if o == 0:
                own[...] = piece
            else:
                diag_send[i, o - 1] = diagonal(piece)
                copy = pltpu.make_async_remote_copy(
                    src_ref=diag_send.at[i, o - 1], dst_ref=diag_recv.at[i, o - 1],
                    send_sem=diag_plane_send.at[i, o - 1], recv_sem=diag_plane_recv.at[i, o - 1],
                    device_id=(q, y), device_id_type=MESH)
                copy.start()
                diag_copies.append(copy)
                send[o - 1] = piece.astype(jnp.bfloat16)
                copy = pltpu.make_async_remote_copy(
                    src_ref=send.at[o - 1], dst_ref=recv.at[o - 1],
                    send_sem=plane_send.at[i, o - 1], recv_sem=plane_recv.at[i, o - 1],
                    device_id=(q, y), device_id_type=MESH)
                copy.start()
                copies.append(copy)
        return copies, diag_copies

    def along_z(copies, own, recv, zsend, zrecv, i):
        copies, diag_copies = copies
        total = own[...]
        diag = diagonal(total)
        for o in range(half - 1):
            diag_copies[o].wait_recv()
            diag = diag + diag_recv[i, o]
            copies[o].wait_recv()
            total = total + recv[o].astype(jnp.float32)
        own[...] = total
        zsend[...] = total.astype(jnp.bfloat16)
        diag_zsend[i] = diag
        out, diag_out = [], []
        for o in range(1, gy):
            z = lax.rem(y + o, gy)
            copy = pltpu.make_async_remote_copy(
                src_ref=diag_zsend.at[i], dst_ref=diag_zrecv.at[i, o - 1],
                send_sem=diag_z_send.at[i, o - 1], recv_sem=diag_z_recv.at[i, o - 1],
                device_id=(x, z), device_id_type=MESH)
            copy.start()
            diag_out.append(copy)
            copy = pltpu.make_async_remote_copy(
                src_ref=zsend.at[tile_rows(z, rows), :], dst_ref=zrecv.at[o - 1],
                send_sem=z_send.at[i, o - 1], recv_sem=z_recv.at[i, o - 1],
                device_id=(x, z), device_id_type=MESH)
            copy.start()
            out.append(copy)
        return out, diag_out

    early_swap.wait_recv()
    early_copies = gram_pieces(early_pair, early_own, early_send, early_recv, 0)

    wait_bytes(late_pair.at[pl.ds(0, tokens - rows), pl.ds(0, cols)], a2a_recv.at[0])
    values = late_pair[:, pl.ds(0, cols)].astype(jnp.float32)
    mean = jnp.sum(values, axis=0, keepdims=True) / tokens
    late_pair[:, pl.ds(0, cols)] = (values - mean).astype(jnp.bfloat16)
    late_swap = swap(late_pair, 1)
    late_swap.start()
    means[:, lanes(me)] = jnp.concatenate([early_mean, mean], axis=0)
    others(lambda t: pltpu.make_async_remote_copy(
        src_ref=means.at[:, lanes(me)], dst_ref=means.at[:, lanes(me)],
        send_sem=mean_send, recv_sem=mean_recv,
        device_id=device(t), device_id_type=MESH).start())

    for copy in plane_copies:
        copy.wait_recv()
    for o in range(1, gy):
        z = lax.rem(y + o, gy)
        for p in range(gx):
            pltpu.make_async_remote_copy(
                src_ref=early_plane.at[tile_rows(z, rows), pl.ds(p * cols, cols)],
                dst_ref=early_out.at[:, lanes(p * gy + y)],
                send_sem=a2a_send.at[1], recv_sem=a2a_recv.at[1],
                device_id=(x, z), device_id_type=MESH).start()
    for p in range(gx):
        pltpu.make_async_copy(
            early_plane.at[tile_rows(y, rows), pl.ds(p * cols, cols)],
            early_out.at[:, lanes(p * gy + y)], own_sem).start()

    late_swap.wait_recv()
    late_copies = gram_pieces(late_pair, late_own, late_send, late_recv, 1)

    early_z = along_z(early_copies, early_own, early_recv, early_zsend, early_zrecv, 0)
    late_z = along_z(late_copies, late_own, late_recv, late_zsend, late_zrecv, 1)

    def final(copies, own, zrecv, i):
        copies, diag_copies = copies
        total = own[tile_rows(y, rows), :]
        diag = diag_zsend[i]
        for o in range(gy - 1):
            diag_copies[o].wait_recv()
            diag = diag + diag_zrecv[i, o]
            copies[o].wait_recv()
            total = total + zrecv[o].astype(jnp.float32)
        first = jnp.where(lane == y * rows + sub, diag, total[:, :block])
        return jnp.concatenate([first, total[:, block:]], axis=1)

    sub = lax.broadcasted_iota(jnp.int32, (rows, block), 0)
    lane = lax.broadcasted_iota(jnp.int32, (rows, block), 1)
    k = final(early_z, early_own, early_zrecv, 0)
    l = final(late_z, late_own, late_zrecv, 1)
    kl = k * l

    def weighted(v):
        doubled = jnp.sum(v[:, block:half * block])
        return jnp.sum(v[:, :block]) + jnp.sum(v[:, half * block:]) + 2.0 * doubled

    head = lax.broadcasted_iota(jnp.int32, (1, block), 1)
    scalars = jnp.where(head == 0, weighted(kl), jnp.where(
        head == 1, weighted(k * k), jnp.where(head == 2, weighted(l * l), 0.0)))
    for d in range(gx):
        if 0 < d < half:
            top = jnp.sum(kl[:, d * block:(d + 1) * block], axis=0, keepdims=True)
        else:
            top = jnp.zeros((1, block), jnp.float32)
        msg[d] = jnp.concatenate([top, scalars], axis=0)
    msg_recv[me] = msg[0]
    others(lambda t: pltpu.make_async_remote_copy(
        src_ref=msg.at[lax.rem(t // gy - x + gx, gx)], dst_ref=msg_recv.at[me],
        send_sem=msg_send, recv_sem=msg_recv_sem,
        device_id=device(t), device_id_type=MESH).start())
    wait_bytes(means.at[:, pl.ds(0, (n - 1) * cols)], mean_recv)
    early_mean_out[...] = means[0:1, :]
    late_mean_out[...] = means[1:2, :]
    own_align = jnp.sum(kl, axis=1, keepdims=True)
    wait_bytes(msg_recv.at[pl.ds(0, n - 1)], msg_recv_sem)
    got = jnp.sum(msg_recv[...], axis=0)
    below = jnp.sum(jnp.where(lane == y * rows + sub, got[0:1, :], 0.0), axis=1, keepdims=True)
    align = jnp.sum(jnp.where(lane == sub, own_align + below, 0.0), axis=0, keepdims=True)
    sums = got[1:2, :]
    total_kl = jnp.sum(jnp.where(head == 0, sums, 0.0), axis=1, keepdims=True)
    total_kk = jnp.sum(jnp.where(head == 1, sums, 0.0), axis=1, keepdims=True)
    total_ll = jnp.sum(jnp.where(head == 2, sums, 0.0), axis=1, keepdims=True)
    scale_norm = jnp.sqrt(total_kk * total_ll)
    share_out[...] = (tokens * align / scale_norm)[:, :rows]
    similarity_out[...] = total_kl / scale_norm

    part = late_pair.at[pl.ds(0, tokens - rows), pl.ds(0, cols)]
    wait_bytes(part, a2a_send.at[0])
    for copy in plane_copies:
        copy.wait_send()
    wait_bytes(early_out.at[:, pl.ds(0, (gy - 1) * gx * cols)], a2a_send.at[1])
    wait_bytes(early_out.at[:, pl.ds(0, (gy - 1) * gx * cols)], a2a_recv.at[1])
    wait_bytes(early_out.at[:, pl.ds(0, gx * cols)], own_sem)
    early_swap.wait_send()
    late_swap.wait_send()
    wait_bytes(means.at[:, pl.ds(0, (n - 1) * cols)], mean_send)
    wait_bytes(msg_recv.at[pl.ds(0, n - 1)], msg_send)
    for copies in (early_copies, late_copies, early_z, late_z):
        for copy in copies[0] + copies[1]:
            copy.wait_send()


def exchange_body(gx, gy, layer_early, layer_late):
    tokens, cols = layer_early.shape
    rows, width = layer_late.shape
    n = gx * gy
    block = tokens // gx
    half = gx // 2
    span = (half + 1) * block
    bf16, f32 = jnp.bfloat16, jnp.float32
    dma = pltpu.SemaphoreType.DMA
    gram = [
        pltpu.VMEM((half - 1, block, span), bf16),
        pltpu.VMEM((half - 1, block, span), bf16),
        pltpu.VMEM((block, span), f32),
    ]
    z_part = [pltpu.VMEM((block, span), bf16), pltpu.VMEM((gy - 1, rows, span), bf16)]
    vmem = pl.BlockSpec(memory_space=pltpu.VMEM)
    anywhere = pl.BlockSpec(memory_space=pl.ANY)
    early_raw, early_mean, late_mean, share, similarity = pl.pallas_call(
        functools.partial(kernel, gx, gy),
        out_shape=(
            jax.ShapeDtypeStruct((rows, width), bf16),
            jax.ShapeDtypeStruct((1, width), f32),
            jax.ShapeDtypeStruct((1, width), f32),
            jax.ShapeDtypeStruct((1, rows), f32),
            jax.ShapeDtypeStruct((1, 1), f32),
        ),
        in_specs=[anywhere, anywhere],
        out_specs=(anywhere, vmem, vmem, vmem, vmem),
        scratch_shapes=[
            pltpu.VMEM((tokens, cols), bf16),
            pltpu.VMEM((rows, width), bf16),
            pltpu.VMEM((block, gx * cols), bf16),
            pltpu.VMEM((tokens, 2 * cols), bf16),
            pltpu.VMEM((tokens, 2 * cols), bf16),
            pltpu.VMEM((2, width), f32),
            *gram, *gram, *z_part, *z_part,
            pltpu.VMEM((2, half - 1, 1, block), f32),
            pltpu.VMEM((2, half - 1, 1, block), f32),
            pltpu.VMEM((2, 1, block), f32),
            pltpu.VMEM((2, gy - 1, 1, block), f32),
            pltpu.VMEM((gx, 2, block), f32),
            pltpu.VMEM((n, 2, block), f32),
            dma((2,)), dma((2,)), dma((2,)), dma, dma((2,)), dma((2,)), dma, dma,
            dma((2, half - 1)), dma((2, half - 1)), dma((2, gy - 1)), dma((2, gy - 1)), dma, dma,
            dma((2, half - 1)), dma((2, half - 1)), dma((2, gy - 1)), dma((2, gy - 1)),
            dma((gx - 1,)), dma((gx - 1,)),
        ],
        compiler_params=pltpu.CompilerParams(collective_id=0, has_side_effects=True),
    )(layer_early, layer_late)
    early_rows = (early_raw.astype(f32) - early_mean).astype(bf16)
    late_rows = (layer_late.astype(f32) - late_mean).astype(bf16)
    return similarity[0, 0], share[0], early_rows, late_rows


def fits(gx, gy, tokens, width):
    n = gx * gy
    cols, rows, block = width // n, tokens // n, tokens // gx
    aligned = cols % 128 == 0 and rows % 16 == 0 and block % 128 == 0
    span = (gx // 2 + 1) * block
    held = 20 * tokens * cols + 4 * gx * block * span + 24 * block * span
    return gx % 2 == 0 and gx >= 4 and gy >= 2 and aligned and rows <= block and held <= VMEM_BUDGET


def solution(mesh):
    gx, gy = mesh.shape["gx"], mesh.shape["gy"]

    def body(layer_early, layer_late):
        if fits(gx, gy, layer_early.shape[0], layer_late.shape[1]):
            return exchange_body(gx, gy, layer_early, layer_late)
        return gather_body(layer_early, layer_late)

    in_specs = (P(None, ("gx", "gy")), P(("gx", "gy"), None))
    out_specs = (P(), P(("gx", "gy")), P(("gx", "gy"), None), P(("gx", "gy"), None))
    return jax.shard_map(body, mesh=mesh, in_specs=in_specs, out_specs=out_specs, check_vma=False)
```

```python
import functools

import jax
import jax.numpy as jnp
from jax import lax
from jax.experimental import pallas as pl
from jax.experimental.pallas import tpu as pltpu
from jax.sharding import PartitionSpec as P

MESH = pl.DeviceIdType.MESH
NT = (((1,), (1,)), ((), ()))
VMEM_BUDGET = 48 * 2**20


def pair_terms(left_early, left_late, right_early, right_late):
    block_early = lax.dot_general(left_early, right_early, NT, preferred_element_type=jnp.float32)
    block_late = lax.dot_general(left_late, right_late, NT, preferred_element_type=jnp.float32)
    return (
        jnp.sum(block_early * block_late, axis=1),
        jnp.sum(block_early * block_early),
        jnp.sum(block_late * block_late),
    )


def gather_body(layer_early, layer_late):
    total_rows = layer_early.shape[0]
    early_values = layer_early.astype(jnp.float32)
    early_cols = (early_values - jnp.mean(early_values, axis=0)).astype(jnp.bfloat16)
    late_values = layer_late.astype(jnp.float32)
    column_sums = lax.psum(jnp.sum(late_values, axis=0), ("gx", "gy"))
    late_rows = (late_values - column_sums / total_rows).astype(jnp.bfloat16)
    early_rows = lax.all_to_all(early_cols, ("gx", "gy"), split_axis=0, concat_axis=1, tiled=True)
    block_early, block_late = (
        lax.all_gather(early_rows, "gy", axis=0, tiled=True),
        lax.all_gather(late_rows, "gy", axis=0, tiled=True),
    )
    row_part, early_part, late_part = pair_terms(
        block_early,
        block_late,
        lax.all_gather(early_rows, "gx", axis=0, tiled=True),
        lax.all_gather(late_rows, "gx", axis=0, tiled=True),
    )
    own_align = lax.psum_scatter(row_part, "gy", scatter_dimension=0, tiled=True)
    total_kl, total_kk, total_ll = lax.psum(
        (jnp.sum(row_part), early_part, late_part), ("gx", "gy")
    )
    scale_norm = jnp.sqrt(total_kk * total_ll)
    similarity = total_kl / scale_norm
    token_share = total_rows * own_align / scale_norm
    return (similarity, token_share, early_rows, late_rows)


def kernel(gx, gy, early_hbm, late_hbm, early_out, early_mean_out, late_mean_out, share_out, similarity_out,
           early_ref, late_ref, early_plane, early_pair, late_pair, means,
           early_send, early_recv, early_own, late_send, late_recv, late_own,
           early_zsend, early_zrecv, late_zsend, late_zrecv,
           diag_send, diag_recv, diag_zsend, diag_zrecv,
           msg, msg_recv,
           stage_sem, a2a_send, a2a_recv, own_sem, pair_send, pair_recv, mean_send, mean_recv,
           plane_send, plane_recv, z_send, z_recv, msg_send, msg_recv_sem,
           diag_plane_send, diag_plane_recv, diag_z_send, diag_z_recv, out_send, out_recv):
    n = gx * gy
    tokens, cols = early_ref.shape
    rows = late_ref.shape[0]
    block = tokens // gx
    half = gx // 2
    x, y = lax.axis_index("gx"), lax.axis_index("gy")
    me = x * gy + y
    core = lax.rem(x, 2)
    chip = x // 2
    partner = x + 1 - 2 * core

    def device(t):
        return (t // gy, lax.rem(t, gy))

    def lanes(i):
        return pl.ds(pl.multiple_of(i * cols, cols), cols)

    def tile_rows(i, size):
        return pl.ds(pl.multiple_of(i * size, size), size)

    def others(f):
        def step(o, carry):
            f(lax.rem(me + o, n))
            return carry
        lax.fori_loop(1, n, step, 0)

    def wait_bytes(ref, sem):
        pltpu.make_async_copy(ref, ref, sem).wait()

    barrier = pltpu.get_barrier_semaphore()
    others(lambda t: pl.semaphore_signal(barrier, inc=1, device_id=device(t), device_id_type=MESH))
    stage_late = pltpu.make_async_copy(late_hbm, late_ref, stage_sem.at[0])
    stage_late.start()
    stage_early = pltpu.make_async_copy(early_hbm, early_ref, stage_sem.at[1])
    stage_early.start()
    stage_late.wait()
    pl.semaphore_wait(barrier, n - 1)

    own_rows = tile_rows(me, rows)

    others(lambda t: pltpu.make_async_remote_copy(
        src_ref=late_ref.at[:, lanes(t)], dst_ref=late_pair.at[own_rows, pl.ds(0, cols)],
        send_sem=a2a_send.at[0], recv_sem=a2a_recv.at[0],
        device_id=device(t), device_id_type=MESH).start())
    late_pair[own_rows, pl.ds(0, cols)] = late_ref[:, lanes(me)]

    stage_early.wait()
    plane_copies = []
    for o in range(1, gx):
        p = lax.rem(x + o, gx)
        copy = pltpu.make_async_remote_copy(
            src_ref=early_ref.at[tile_rows(p, block), :], dst_ref=early_plane.at[:, lanes(x)],
            send_sem=out_send.at[o - 1], recv_sem=out_recv.at[o - 1],
            device_id=(p, y), device_id_type=MESH)
        copy.start()
        plane_copies.append(copy)
    early_plane[:, lanes(x)] = early_ref[tile_rows(x, block), :]

    values = early_ref[...].astype(jnp.float32)
    early_mean = jnp.sum(values, axis=0, keepdims=True) / tokens
    early_pair[:, pl.ds(0, cols)] = (values - early_mean).astype(jnp.bfloat16)

    def swap(pair, i):
        return pltpu.make_async_remote_copy(
            src_ref=pair.at[:, pl.ds(0, cols)], dst_ref=pair.at[:, pl.ds(cols, cols)],
            send_sem=pair_send.at[i], recv_sem=pair_recv.at[i],
            device_id=(partner, y), device_id_type=MESH)

    early_swap = swap(early_pair, 0)
    early_swap.start()

    def diagonal(v):
        on = (lax.broadcasted_iota(jnp.int32, (block, block), 0)
              == lax.broadcasted_iota(jnp.int32, (block, block), 1))
        return jnp.sum(jnp.where(on, v[:, :block], 0.0), axis=0, keepdims=True)

    def gram_pieces(pair, own, send, recv, i):
        copies, diag_copies = [], []
        for o in list(range(1, half)) + [0]:
            q = 2 * lax.rem(chip + o, half) + core
            left = pair[tile_rows(q, block), :]
            right = jnp.concatenate(
                [pair[tile_rows(lax.rem(q + d, gx), block), :] for d in range(half + 1)], axis=0)
            piece = lax.dot_general(left, right, NT, preferred_element_type=jnp.float32)
            if o == 0:
                own[...] = piece
            else:
                diag_send[i, o - 1] = diagonal(piece)
                copy = pltpu.make_async_remote_copy(
                    src_ref=diag_send.at[i, o - 1], dst_ref=diag_recv.at[i, o - 1],
                    send_sem=diag_plane_send.at[i, o - 1], recv_sem=diag_plane_recv.at[i, o - 1],
                    device_id=(q, y), device_id_type=MESH)
                copy.start()
                diag_copies.append(copy)
                send[o - 1] = piece.astype(jnp.bfloat16)
                copy = pltpu.make_async_remote_copy(
                    src_ref=send.at[o - 1], dst_ref=recv.at[o - 1],
                    send_sem=plane_send.at[i, o - 1], recv_sem=plane_recv.at[i, o - 1],
                    device_id=(q, y), device_id_type=MESH)
                copy.start()
                copies.append(copy)
        return copies, diag_copies

    def along_z(copies, own, recv, zsend, zrecv, i):
        copies, diag_copies = copies
        total = own[...]
        diag = diagonal(total)
        for o in range(half - 1):
            diag_copies[o].wait_recv()
            diag = diag + diag_recv[i, o]
            copies[o].wait_recv()
            total = total + recv[o].astype(jnp.float32)
        own[...] = total
        zsend[...] = total.astype(jnp.bfloat16)
        diag_zsend[i] = diag
        out, diag_out = [], []
        for o in range(1, gy):
            z = lax.rem(y + o, gy)
            copy = pltpu.make_async_remote_copy(
                src_ref=diag_zsend.at[i], dst_ref=diag_zrecv.at[i, o - 1],
                send_sem=diag_z_send.at[i, o - 1], recv_sem=diag_z_recv.at[i, o - 1],
                device_id=(x, z), device_id_type=MESH)
            copy.start()
            diag_out.append(copy)
            copy = pltpu.make_async_remote_copy(
                src_ref=zsend.at[tile_rows(z, rows), :], dst_ref=zrecv.at[o - 1],
                send_sem=z_send.at[i, o - 1], recv_sem=z_recv.at[i, o - 1],
                device_id=(x, z), device_id_type=MESH)
            copy.start()
            out.append(copy)
        return out, diag_out

    early_swap.wait_recv()
    early_copies = gram_pieces(early_pair, early_own, early_send, early_recv, 0)

    wait_bytes(late_pair.at[pl.ds(0, tokens - rows), pl.ds(0, cols)], a2a_recv.at[0])
    values = late_pair[:, pl.ds(0, cols)].astype(jnp.float32)
    mean = jnp.sum(values, axis=0, keepdims=True) / tokens
    late_pair[:, pl.ds(0, cols)] = (values - mean).astype(jnp.bfloat16)
    late_swap = swap(late_pair, 1)
    late_swap.start()
    means[:, lanes(me)] = jnp.concatenate([early_mean, mean], axis=0)
    others(lambda t: pltpu.make_async_remote_copy(
        src_ref=means.at[:, lanes(me)], dst_ref=means.at[:, lanes(me)],
        send_sem=mean_send, recv_sem=mean_recv,
        device_id=device(t), device_id_type=MESH).start())

    for copy in plane_copies:
        copy.wait_recv()
    for o in range(1, gy):
        z = lax.rem(y + o, gy)
        for p in range(gx):
            pltpu.make_async_remote_copy(
                src_ref=early_plane.at[tile_rows(z, rows), pl.ds(p * cols, cols)],
                dst_ref=early_out.at[:, lanes(p * gy + y)],
                send_sem=a2a_send.at[1], recv_sem=a2a_recv.at[1],
                device_id=(x, z), device_id_type=MESH).start()
    for p in range(gx):
        pltpu.make_async_copy(
            early_plane.at[tile_rows(y, rows), pl.ds(p * cols, cols)],
            early_out.at[:, lanes(p * gy + y)], own_sem).start()

    late_swap.wait_recv()
    late_copies = gram_pieces(late_pair, late_own, late_send, late_recv, 1)

    early_z = along_z(early_copies, early_own, early_recv, early_zsend, early_zrecv, 0)
    late_z = along_z(late_copies, late_own, late_recv, late_zsend, late_zrecv, 1)

    def final(copies, own, zrecv, i):
        copies, diag_copies = copies
        total = own[tile_rows(y, rows), :]
        diag = diag_zsend[i]
        for o in range(gy - 1):
            diag_copies[o].wait_recv()
            diag = diag + diag_zrecv[i, o]
            copies[o].wait_recv()
            total = total + zrecv[o].astype(jnp.float32)
        first = jnp.where(lane == y * rows + sub, diag, total[:, :block])
        return jnp.concatenate([first, total[:, block:]], axis=1)

    sub = lax.broadcasted_iota(jnp.int32, (rows, block), 0)
    lane = lax.broadcasted_iota(jnp.int32, (rows, block), 1)
    k = final(early_z, early_own, early_zrecv, 0)
    def weighted(v):
        doubled = jnp.sum(v[:, block:half * block])
        return jnp.sum(v[:, :block]) + jnp.sum(v[:, half * block:]) + 2.0 * doubled

    kk = weighted(k * k)
    l = final(late_z, late_own, late_zrecv, 1)
    kl = k * l

    head = lax.broadcasted_iota(jnp.int32, (1, block), 1)
    scalars = jnp.where(head == 0, weighted(kl), jnp.where(
        head == 1, kk, jnp.where(head == 2, weighted(l * l), 0.0)))
    for d in range(gx):
        if 0 < d < half:
            top = jnp.sum(kl[:, d * block:(d + 1) * block], axis=0, keepdims=True)
        else:
            top = jnp.zeros((1, block), jnp.float32)
        msg[d] = jnp.concatenate([top, scalars], axis=0)
    msg_recv[me] = msg[0]
    others(lambda t: pltpu.make_async_remote_copy(
        src_ref=msg.at[lax.rem(t // gy - x + gx, gx)], dst_ref=msg_recv.at[me],
        send_sem=msg_send, recv_sem=msg_recv_sem,
        device_id=device(t), device_id_type=MESH).start())
    wait_bytes(means.at[:, pl.ds(0, (n - 1) * cols)], mean_recv)
    early_mean_out[...] = means[0:1, :]
    late_mean_out[...] = means[1:2, :]
    own_align = jnp.sum(kl, axis=1, keepdims=True)
    wait_bytes(msg_recv.at[pl.ds(0, n - 1)], msg_recv_sem)
    got = jnp.sum(msg_recv[...], axis=0)
    below = jnp.sum(jnp.where(lane == y * rows + sub, got[0:1, :], 0.0), axis=1, keepdims=True)
    align = jnp.sum(jnp.where(lane == sub, own_align + below, 0.0), axis=0, keepdims=True)
    sums = got[1:2, :]
    total_kl = jnp.sum(jnp.where(head == 0, sums, 0.0), axis=1, keepdims=True)
    total_kk = jnp.sum(jnp.where(head == 1, sums, 0.0), axis=1, keepdims=True)
    total_ll = jnp.sum(jnp.where(head == 2, sums, 0.0), axis=1, keepdims=True)
    scale_norm = jnp.sqrt(total_kk * total_ll)
    share_out[...] = (tokens * align / scale_norm)[:, :rows]
    similarity_out[...] = total_kl / scale_norm

    part = late_pair.at[pl.ds(0, tokens - rows), pl.ds(0, cols)]
    wait_bytes(part, a2a_send.at[0])
    for copy in plane_copies:
        copy.wait_send()
    wait_bytes(early_out.at[:, pl.ds(0, (gy - 1) * gx * cols)], a2a_send.at[1])
    wait_bytes(early_out.at[:, pl.ds(0, (gy - 1) * gx * cols)], a2a_recv.at[1])
    wait_bytes(early_out.at[:, pl.ds(0, gx * cols)], own_sem)
    early_swap.wait_send()
    late_swap.wait_send()
    wait_bytes(means.at[:, pl.ds(0, (n - 1) * cols)], mean_send)
    wait_bytes(msg_recv.at[pl.ds(0, n - 1)], msg_send)
    for copies in (early_copies, late_copies, early_z, late_z):
        for copy in copies[0] + copies[1]:
            copy.wait_send()


def exchange_body(gx, gy, layer_early, layer_late):
    tokens, cols = layer_early.shape
    rows, width = layer_late.shape
    n = gx * gy
    block = tokens // gx
    half = gx // 2
    span = (half + 1) * block
    bf16, f32 = jnp.bfloat16, jnp.float32
    dma = pltpu.SemaphoreType.DMA
    gram = [
        pltpu.VMEM((half - 1, block, span), bf16),
        pltpu.VMEM((half - 1, block, span), bf16),
        pltpu.VMEM((block, span), f32),
    ]
    z_part = [pltpu.VMEM((block, span), bf16), pltpu.VMEM((gy - 1, rows, span), bf16)]
    vmem = pl.BlockSpec(memory_space=pltpu.VMEM)
    anywhere = pl.BlockSpec(memory_space=pl.ANY)
    early_raw, early_mean, late_mean, share, similarity = pl.pallas_call(
        functools.partial(kernel, gx, gy),
        out_shape=(
            jax.ShapeDtypeStruct((rows, width), bf16),
            jax.ShapeDtypeStruct((1, width), f32),
            jax.ShapeDtypeStruct((1, width), f32),
            jax.ShapeDtypeStruct((1, rows), f32),
            jax.ShapeDtypeStruct((1, 1), f32),
        ),
        in_specs=[anywhere, anywhere],
        out_specs=(anywhere, vmem, vmem, vmem, vmem),
        scratch_shapes=[
            pltpu.VMEM((tokens, cols), bf16),
            pltpu.VMEM((rows, width), bf16),
            pltpu.VMEM((block, gx * cols), bf16),
            pltpu.VMEM((tokens, 2 * cols), bf16),
            pltpu.VMEM((tokens, 2 * cols), bf16),
            pltpu.VMEM((2, width), f32),
            *gram, *gram, *z_part, *z_part,
            pltpu.VMEM((2, half - 1, 1, block), f32),
            pltpu.VMEM((2, half - 1, 1, block), f32),
            pltpu.VMEM((2, 1, block), f32),
            pltpu.VMEM((2, gy - 1, 1, block), f32),
            pltpu.VMEM((gx, 2, block), f32),
            pltpu.VMEM((n, 2, block), f32),
            dma((2,)), dma((2,)), dma((2,)), dma, dma((2,)), dma((2,)), dma, dma,
            dma((2, half - 1)), dma((2, half - 1)), dma((2, gy - 1)), dma((2, gy - 1)), dma, dma,
            dma((2, half - 1)), dma((2, half - 1)), dma((2, gy - 1)), dma((2, gy - 1)),
            dma((gx - 1,)), dma((gx - 1,)),
        ],
        compiler_params=pltpu.CompilerParams(collective_id=0, has_side_effects=True),
    )(layer_early, layer_late)
    early_rows = (early_raw.astype(f32) - early_mean).astype(bf16)
    late_rows = (layer_late.astype(f32) - late_mean).astype(bf16)
    return similarity[0, 0], share[0], early_rows, late_rows


def fits(gx, gy, tokens, width):
    n = gx * gy
    cols, rows, block = width // n, tokens // n, tokens // gx
    aligned = cols % 128 == 0 and rows % 16 == 0 and block % 128 == 0
    span = (gx // 2 + 1) * block
    held = 20 * tokens * cols + 4 * gx * block * span + 24 * block * span
    return gx % 2 == 0 and gx >= 4 and gy >= 2 and aligned and rows <= block and held <= VMEM_BUDGET


def solution(mesh):
    gx, gy = mesh.shape["gx"], mesh.shape["gy"]

    def body(layer_early, layer_late):
        if fits(gx, gy, layer_early.shape[0], layer_late.shape[1]):
            return exchange_body(gx, gy, layer_early, layer_late)
        return gather_body(layer_early, layer_late)

    in_specs = (P(None, ("gx", "gy")), P(("gx", "gy"), None))
    out_specs = (P(), P(("gx", "gy")), P(("gx", "gy"), None), P(("gx", "gy"), None))
    return jax.shard_map(body, mesh=mesh, in_specs=in_specs, out_specs=out_specs, check_vma=False)
```
